32 devices in a mesh: member: 1 (over z), ty: 4 (over y), tx: 4 (over x), panel: 2 (over core).
Axes of the slice: x: 4, y: 4, z: 1, core: 2. Of those that a mesh axis runs over, the one named last changes fastest.
The devices are a block of a 4x4x8 slice.
Arguments:
- tracer: float32 [6, 720, 720], P(('member', 'panel'), 'tx', 'ty')
- wind_a: float32 [6, 720, 720], P('panel', 'tx', 'ty')
- wind_b: float32 [6, 720, 720], P('panel', 'tx', 'ty')
- wind_scale: float32 [64], replicated
Outputs:
- output: float32 [6, 720, 720], P(('member', 'panel'), 'tx', 'ty')
All inputs are finite; a program needn't handle non-finite values.
Results may differ from the reference program's by a relative error of at most 0.001.
Values sent between devices are 32-bit elements.
A program may use at most 768 MiB of HBM per device.

```python
import math
import jax
import jax.numpy as jnp
from jax import lax

N = 720
STEPS = 64

C_SPEED = 2.5
CFL_STEP = 0.12
DALPHA = 0.5 * math.pi / N
DT = CFL_STEP * DALPHA
EDGE_TABLE = (
    ((3, 1, 0), (1, 0, 0), (5, 3, 0), (4, 2, 0)),
    ((0, 1, 0), (2, 0, 0), (5, 1, 1), (4, 1, 0)),
    ((1, 1, 0), (3, 0, 0), (5, 2, 1), (4, 3, 1)),
    ((2, 1, 0), (0, 0, 0), (5, 0, 0), (4, 0, 1)),
    ((3, 3, 1), (1, 3, 0), (0, 3, 0), (2, 3, 1)),
    ((3, 2, 0), (1, 2, 1), (2, 2, 1), (0, 2, 0)),
)
TANGENT_A = ((0.0, 1.0, 0.0), (-1.0, 0.0, 0.0), (0.0, -1.0, 0.0), (1.0, 0.0, 0.0), (0.0, 1.0, 0.0), (0.0, 1.0, 0.0))
TANGENT_B = ((0.0, 0.0, 1.0), (0.0, 0.0, 1.0), (0.0, 0.0, 1.0), (0.0, 0.0, 1.0), (-1.0, 0.0, 0.0), (1.0, 0.0, 0.0))


def edge_sign(side_id, edge_id):
    out_sign = 1.0 if edge_id in (1, 3) else -1.0
    return out_sign if side_id in (0, 2) else -out_sign


def out_strips(field_a, field_b):
    return (field_a[:, 0:2, :],
            jnp.flip(field_a[:, -2:, :], axis=1),
            jnp.swapaxes(field_b[:, :, 0:2], 1, 2),
            jnp.swapaxes(jnp.flip(field_b[:, :, -2:], axis=2), 1, 2))


def to_blocks(ghosts):
    return (jnp.flip(ghosts[0], axis=1), ghosts[1],
            jnp.swapaxes(jnp.flip(ghosts[2], axis=1), 1, 2), jnp.swapaxes(ghosts[3], 1, 2))


def sphere_blocks(field_a, field_b, signed):
    strips = out_strips(field_a, field_b)
    ghosts = []
    for side_id in range(4):
        per_panel = []
        for panel_id in range(6):
            src_panel, edge_id, flipped = EDGE_TABLE[panel_id][side_id]
            one_strip = strips[edge_id][src_panel]
            if flipped:
                one_strip = jnp.flip(one_strip, axis=1)
            if signed:
                one_strip = edge_sign(side_id, edge_id) * one_strip
            per_panel.append(one_strip)
        ghosts.append(jnp.stack(per_panel))
    return to_blocks(ghosts)


def extend_field(field_now, blocks):
    return (jnp.concatenate([blocks[0], field_now, blocks[1]], axis=1),
            jnp.concatenate([blocks[2], field_now, blocks[3]], axis=2))


def wind_faces(blocks, wind_a, wind_b):
    ext_a = jnp.concatenate([blocks[0][:, 1:2, :], wind_a, blocks[1][:, 0:1, :]], axis=1)
    ext_b = jnp.concatenate([blocks[2][:, :, 1:2], wind_b, blocks[3][:, :, 0:1]], axis=2)
    return 0.5 * (ext_a[:, :-1, :] + ext_a[:, 1:, :]), 0.5 * (ext_b[:, :, :-1] + ext_b[:, :, 1:])


def face_flux_div(ext_arr, wind_face, step_scale, axis_id):
    face_count = ext_arr.shape[axis_id] - 3
    far_left = lax.slice_in_dim(ext_arr, 0, face_count, axis=axis_id)
    near_left = lax.slice_in_dim(ext_arr, 1, face_count + 1, axis=axis_id)
    near_right = lax.slice_in_dim(ext_arr, 2, face_count + 2, axis=axis_id)
    far_right = lax.slice_in_dim(ext_arr, 3, face_count + 3, axis=axis_id)
    face_val = (7.0 * (near_left + near_right) - (far_left + far_right)) / 12.0
    face_flux = step_scale * wind_face * face_val - (0.5 * C_SPEED) * (near_right - near_left)
    return (lax.slice_in_dim(face_flux, 1, face_count, axis=axis_id)
            - lax.slice_in_dim(face_flux, 0, face_count - 1, axis=axis_id))


def tendency(ext_a, ext_b, face_a, face_b, step_scale, inv_area):
    div_total = face_flux_div(ext_a, face_a, step_scale, 1) + face_flux_div(ext_b, face_b, step_scale, 2)
    return -div_total * inv_area


def inverse_area(row_ids, col_ids, cells):
    dalpha = 0.5 * math.pi / cells
    tan_a = jnp.tan((row_ids.astype(jnp.float32) + 0.5) * dalpha - 0.25 * math.pi)[:, None]
    tan_b = jnp.tan((col_ids.astype(jnp.float32) + 0.5) * dalpha - 0.25 * math.pi)[None, :]
    r_sq = 1.0 + tan_a * tan_a + tan_b * tan_b
    sqrt_g = (1.0 + tan_a * tan_a) * (1.0 + tan_b * tan_b) / (r_sq * jnp.sqrt(r_sq))
    return 1.0 / (dalpha * sqrt_g)


def sphere_points():
    centre_tan = jnp.tan((jnp.arange(N, dtype=jnp.float32) + 0.5) * DALPHA - 0.25 * math.pi)
    tan_a = jnp.broadcast_to(centre_tan[:, None], (N, N))
    tan_b = jnp.broadcast_to(centre_tan[None, :], (N, N))
    ones_grid = jnp.ones((N, N), jnp.float32)
    comp_x = jnp.stack([ones_grid, -tan_a, -ones_grid, tan_a, -tan_b, tan_b])
    comp_y = jnp.stack([tan_a, ones_grid, -tan_a, -ones_grid, tan_a, tan_a])
    comp_z = jnp.stack([tan_b, tan_b, tan_b, tan_b, ones_grid, -ones_grid])
    cube_pts = jnp.stack([comp_x, comp_y, comp_z], axis=-1)
    return tan_a, tan_b, cube_pts / jnp.linalg.norm(cube_pts, axis=-1, keepdims=True)


def flux_winds(tan_a, tan_b, velocity):
    along_a = jnp.sum(velocity * jnp.array(TANGENT_A, jnp.float32)[:, None, None, :], axis=-1)
    along_b = jnp.sum(velocity * jnp.array(TANGENT_B, jnp.float32)[:, None, None, :], axis=-1)
    sq_a = tan_a * tan_a
    sq_b = tan_b * tan_b
    r_sq = 1.0 + sq_a + sq_b
    cross_ab = tan_a * tan_b
    wind_a = (1.0 + sq_b) * ((1.0 + sq_a) * along_a + cross_ab * along_b) / r_sq
    wind_b = (1.0 + sq_a) * (cross_ab * along_a + (1.0 + sq_b) * along_b) / r_sq
    return wind_a, wind_b


def random_unit(key_vec):
    raw_vec = jax.random.normal(key_vec, (3,), jnp.float32)
    return raw_vec / jnp.linalg.norm(raw_vec)


def setup_inputs(seed: int = 0, part: int = 0) -> dict:
    base_key = jax.random.key(seed)
    shared_key, part_key = jax.random.split(base_key)
    part_key = jax.random.fold_in(part_key, part)
    tan_a, tan_b, sphere_pts = sphere_points()
    key_axis, key_rate, key_scale = jax.random.split(shared_key, 3)
    rot_axis = random_unit(key_axis) * jax.random.uniform(key_rate, (), jnp.float32, 0.6, 1.0)
    velocity = jnp.cross(rot_axis, sphere_pts)
    wind_a, wind_b = flux_winds(tan_a, tan_b, velocity)
    wind_scale = jax.random.uniform(key_scale, (STEPS,), jnp.float32, -0.2, 1.0)
    key_front, key_wave, key_phase = jax.random.split(part_key, 3)
    front_part = jnp.tanh((N / 12.0) * (sphere_pts @ random_unit(key_front)))
    wave_phase = jax.random.uniform(key_phase, (), jnp.float32, 0.0, 2.0 * math.pi)
    wave_part = jnp.sin((N / 6.0) * (sphere_pts @ random_unit(key_wave)) + wave_phase)
    tracer = 0.8 * front_part + 0.5 * wave_part
    return {'tracer': tracer.astype(jnp.float32), 'wind_a': wind_a.astype(jnp.float32),
            'wind_b': wind_b.astype(jnp.float32), 'wind_scale': wind_scale}


def reference(tracer, wind_a, wind_b, wind_scale):
    cell_ids = jnp.arange(N)
    inv_area = inverse_area(cell_ids, cell_ids, N)
    face_a, face_b = wind_faces(sphere_blocks(wind_a, wind_b, True), wind_a, wind_b)

    def tend_of(tracer_now, step_scale):
        ext_a, ext_b = extend_field(tracer_now, sphere_blocks(tracer_now, tracer_now, False))
        return tendency(ext_a, ext_b, face_a, face_b, step_scale, inv_area)

    def one_step(tracer_now, step_scale):
        stage_one = tracer_now + DT * tend_of(tracer_now, step_scale)
        stage_two = stage_one + DT * tend_of(stage_one, step_scale)
        return 0.5 * (tracer_now + stage_two), None

    return lax.scan(one_step, tracer, wind_scale)[0]
```

```python
import functools
import math
import jax
import jax.numpy as jnp
from jax import lax
from jax.experimental import pallas as pl
from jax.experimental.pallas import tpu as pltpu
from jax.sharding import PartitionSpec as P

C_SPEED = 2.5
CFL_STEP = 0.12
EDGES = ('310,100,530,420', '010,200,511,410', '110,300,521,431', '210,000,500,401', '331,130,030,231', '320,121,221,020')
EDGE_TABLE = [[[int(digit) for digit in side] for side in panel.split(',')] for panel in EDGES]

LANES = 128
NV = 16
NW = 4
OFF = 38
HALO = 32
STEPS_PER_ROUND = 8
NIBBLE = 4
SUBS = 8
HALF = 64
PAIR = range(2)
QUADS = range(4)
ORDERS = {'a': '210', 'b': '201', 'c': '120', 'd': '102'}
ORDER_OF = 'abbbaaaacccccccc' + 'bacdbacdbacdaacd'
F32 = jnp.float32
I32 = jnp.int32
MESH_ID = pl.DeviceIdType.MESH


def lane_id():
    return lax.broadcasted_iota(I32, (SUBS, LANES), 1)


def sub_id():
    return lax.broadcasted_iota(I32, (SUBS, LANES), 0)


def lanes_of(val, idx):
    return jnp.take_along_axis(val, idx, axis=1, mode="promise_in_bounds")


def rev8(val):
    return jnp.take_along_axis(val, 7 - sub_id(), axis=0, mode="promise_in_bounds")


def pick(sel, vals):
    if isinstance(sel, int):
        return vals[sel]
    out = vals[-1]
    for i in range(len(vals) - 2, -1, -1):
        out = jnp.where(sel == i, vals[i], out)
    return out


def reg(v):
    return pl.ds(SUBS * v, SUBS)


def at(pos):
    return pl.ds(pos, SUBS)


def nat(t):
    return pl.ds(HALF * (t & 1) + (t >> 1), 8, stride=8)


class Where:
    def __init__(self, tiles, panels_per_dev):
        self.n, self.lp = tiles, panels_per_dev
        self.tx, self.ty, self.pd = lax.axis_index('tx'), lax.axis_index('ty'), lax.axis_index('panel')
        self.ftx, self.fty = self.flip(self.tx), self.flip(self.ty)
        self.edge_x = self.at_edge(self.tx)
        self.edge_y = self.at_edge(self.ty)
        self.vertex = self.edge_x * self.edge_y

    def flip(self, t):
        return lax.div(t, jnp.int32(self.n // 2))

    def at_edge(self, t):
        return jnp.where(t == 0, 1, jnp.where(t == self.n - 1, 1, 0))

    @staticmethod
    def xor(a, b):
        return a + b - 2 * a * b

    def lookup(self, panel, base, bit):
        code = None
        for p in range(6):
            lo, hi = (np * 8 + e * 2 + fl for np, e, fl in (EDGE_TABLE[p][base], EDGE_TABLE[p][base + 1]))
            val = lo + bit * (hi - lo)
            code = val if code is None else jnp.where(panel == p, val, code)
        return code

    def cross(self, slot, base, bit, along, along_half):
        code = self.lookup(self.lp * self.pd + slot, base, bit)
        np_, e, fl = code >> 3, (code >> 1) & 3, code & 1
        al = along + fl * (self.n - 1 - 2 * along)
        alh = self.xor(along_half, fl)
        col, end = e >> 1, e & 1
        far = end * (self.n - 1)
        tx = far + col * (al - far)
        ty = al + col * (far - al)
        hp = end + col * (alh - end)
        kp = alh + col * (end - alh)
        pd = lax.div(np_, jnp.int32(self.lp))
        return (pd, np_ - pd * self.lp, tx, ty, self.xor(hp, self.flip(tx)), self.xor(kp, self.flip(ty)), col)

    def mix(self, flag, a, b):
        return tuple(x + flag * (y - x) for x, y in zip(a, b))

    def face(self, slot, h, k, kind):
        hp, kp = self.xor(h, self.ftx), self.xor(k, self.fty)
        if kind == 0:
            tx = self.tx + 2 * hp - 1
            inner = (self.pd, slot, tx, self.ty, self.xor(1 - hp, self.flip(tx)), k, 0)
            return self.mix((1 - h) * self.edge_x, inner, self.cross(slot, 0, hp, self.ty, kp))
        ty = self.ty + 2 * kp - 1
        inner = (self.pd, slot, self.tx, ty, h, self.xor(1 - kp, self.flip(ty)), 1)
        return self.mix((1 - k) * self.edge_y, inner, self.cross(slot, 2, kp, self.tx, hp))

    def corner(self, slot, h, k):
        hp, kp = self.xor(h, self.ftx), self.xor(k, self.fty)
        tx, ty = self.tx + 2 * hp - 1, self.ty + 2 * kp - 1
        dest = (self.pd, slot, tx, ty, self.xor(1 - hp, self.flip(tx)), self.xor(1 - kp, self.flip(ty)), 0)
        d = self.cross(slot, 2, kp, tx, 1 - hp)
        dest = self.mix((1 - k) * self.edge_y, dest, d[:6] + (1 - d[6],))
        return self.mix((1 - h) * self.edge_x, dest, self.cross(slot, 0, hp, ty, 1 - kp))


def kernel(tiles, steps, size, ws, in_ref, k_in, out, st, xb, fr, fc, fcm, kk, mm, vcoef, vbuf, vcol, vrow, roll_buf, row_buf, nat_buf, turn,
           strip, strip_c, rbuf, rbuf_c, send_sem, recv_sem):
    slots = out.shape[0]
    lane, sub = lane_id(), sub_id()
    lb, half = lane & 63, lane >> 6
    here = Where(tiles, slots)
    rounds = steps // STEPS_PER_ROUND
    vertex = here.vertex == 1

    def loop(count, fn, first=0):
        def body(i, carry):
            fn(i)
            return carry
        lax.fori_loop(first, count, body, 0)

    def plan(slot, qd, kind):
        h, k = qd >> 1, qd & 1
        dest = here.corner(slot, h, k) if kind == 2 else here.face(slot, h, k, kind)
        code = dest[0]
        for i, part in enumerate((dest[1], dest[2], dest[3], 2 * dest[4] + dest[5], dest[6])):
            code = code + (part << (NIBBLE * (i + 1)))
        if kind == 2:
            stays = vertex & (qd == 0)
        else:
            stays = (dest[0] == here.pd) & (dest[2] == here.tx) & (dest[3] == here.ty)
        return code + jnp.where(stays, 1 << (6 * NIBBLE), 0)

    plans = [[[plan(slot, qd, kind) for kind in range(3)] for qd in QUADS] for slot in range(slots)]

    def code_of(slot, qd, kind):
        return pick(slot, [plans[i][qd][kind] for i in range(slots)])

    def to(slot, qd, kind):
        code = code_of(slot, qd, kind)
        pd, slot2, tx, ty, qd2, kind2 = [(code >> (NIBBLE * i)) & ((1 << NIBBLE) - 1) for i in range(6)]
        return {'panel': pd, 'tx': tx, 'ty': ty}, slot2, qd2, kind2, (code >> (6 * NIBBLE)) == 1

    def leaves(slot, qd, kind):
        return (code_of(slot, qd, kind) >> (6 * NIBBLE)) == 0

    def send(field, set_id, slot):
        for qd in QUADS:
            for kind in range(3):
                device, slot2, qd2, kind2, stays = to(slot, qd, kind)
                if kind < 2:
                    src, dst = strip.at[field, slot, qd, kind, pl.ds(SUBS, HALO)], rbuf.at[set_id, slot2, qd2, kind2]
                    sem = recv_sem.at[set_id, slot2, qd2, kind2]
                else:
                    src, dst = strip_c.at[field, slot, qd, kind2], rbuf_c.at[set_id, slot2, qd2]
                    sem = recv_sem.at[set_id, slot2, qd2, 2]

                @pl.when(jnp.logical_not(stays))
                def _():
                    pltpu.make_async_remote_copy(
                        src_ref=src, dst_ref=dst, send_sem=send_sem.at[field, slot, qd, kind], recv_sem=sem,
                        device_id=device, device_id_type=MESH_ID).start()

                if kind < 2 and (qd >> 1, qd & 1)[kind] == 0:
                    @pl.when(stays)
                    def _():
                        for g in QUADS:
                            rbuf[set_id, slot2, qd2, kind2, reg(g), :] = (
                                strip[field, slot, qd, kind, at(8 + SUBS * g), :])

    def wait_all(field, set_id, slot, sent):
        for qd in QUADS:
            for kind in range(3):
                if kind < 2:
                    src, dst = strip.at[field, slot, qd, kind, pl.ds(SUBS, HALO)], rbuf.at[set_id, slot, qd, kind]
                else:
                    src, dst = strip_c.at[field, slot, qd, 0], rbuf_c.at[set_id, slot, qd]

                def wait():
                    copy = pltpu.make_async_remote_copy(
                        src_ref=src, dst_ref=dst, send_sem=send_sem.at[field, slot, qd, kind],
                        recv_sem=recv_sem.at[set_id, slot, qd, kind],
                        device_id={'panel': here.pd, 'tx': here.tx, 'ty': here.ty}, device_id_type=MESH_ID)
                    if sent:
                        copy.wait_send()
                    else:
                        copy.wait_recv()

                if (qd == 0) if kind == 2 else ((qd >> 1, qd & 1)[kind] == 0):
                    pl.when(leaves(slot, qd, kind))(wait)
                else:
                    wait()

    def other(field):
        return jnp.where(field == 0, 0, 3 - field)

    def signed(cond):
        return jnp.where(cond, -1.0, 1.0).astype(F32)

    def pack(field, slot):
        row_idx = [[HALF * h + (63 - (lane >> 2) if k else lane >> 2) for k in PAIR] for h in PAIR]
        plane = lane & 3
        sign_r, sign_c = signed(field == 2), signed(field == 1)
        src_c = other(field)

        def rows_out(t):
            rows = [st[field, slot, w, nat(t), :] for w in range(NW)]
            for h in PAIR:
                for k in PAIR:
                    val = pick(3 - plane if k else plane, [lanes_of(v, row_idx[h][k]) for v in rows])
                    strip[field, slot, 2 * h + k, 0, at(SUBS * t - 30), :] = val * sign_r if k else val

        for t in range(4, 9):
            rows_out(t)
        for w in range(NW):
            turned = jnp.concatenate([st[src_c, slot, w, nat(t), :] for t in range(16)], axis=0).T
            for h in PAIR:
                for k, first, start in ((0, 8, 2 + w), (0, 16, 34 + w), (1, 48, 5 - w), (1, 40, 37 - w)):
                    val = turned[HALF * h + first:HALF * h + first + 8, :]
                    strip[field, slot, 2 * h + k, 1, pl.ds(start, 8, stride=4), :] = rev8(val) * sign_c if k else val
        idx = 69 - (lane & 31)
        for qd in QUADS:
            for ver in PAIR:
                vals = [lanes_of(strip[field, slot, qd, ver, at(8 + SUBS * g), :], idx) for g in QUADS]
                strip_c[field, slot, qd, ver] = pick(lane >> 5, vals)

    def unpack(set_id, field, slot):
        dst_c = other(field)
        row_sign = [signed(field == 1), signed(field >= 1)]
        block_sign = [signed(field >= 1), signed(field == 1)]
        col_sign = [signed(field == 1), signed(field < 0)]
        idx = [jnp.where(lb < 32, 4 * lb + w, 255 - 4 * lb - w) for w in range(NW)]
        for g in QUADS:
            vals = []
            for qd in QUADS:
                face = rbuf[set_id, slot, qd, 0, reg(g), :] * row_sign[qd & 1]
                block = pltpu.roll(rbuf_c[set_id, slot, qd], (6 - 32 * g) % LANES, 1) * block_sign[qd & 1]
                vals.append(rev8(jnp.where(lane < OFF, block, face)))
            for w in range(NW):
                nat_buf[w, at(30 - SUBS * g), :] = pick(lane >> 5, [lanes_of(v, idx[w]) for v in vals])
        for w in range(NW):
            for t in range(5):
                val = nat_buf[w, reg(t), :]
                if t == 0:
                    val = jnp.where(sub >= 6, val, 0.0)
                if t == 4:
                    val = jnp.where(sub < 6, val, st[field, slot, w, nat(t), :])
                st[field, slot, w, nat(t), :] = val
        side_sign = jnp.where(lb < 32, col_sign[0], col_sign[1])
        for w in range(NW):
            low = 1 if w >= 2 else 2
            for h in PAIR:
                turn[w, at(HALF * h + low), :] = rev8(
                    rbuf[set_id, slot, 2 * h, 1, pl.ds((1, 0, 3, 2)[w], 8, stride=4), :])
                turn[w, at(HALF * h + 53 + low), :] = (
                    rbuf[set_id, slot, 2 * h + 1, 1, pl.ds((2, 3, 0, 1)[w], 8, stride=4), :])
            turned = turn[w].T
            inside = ((lb >= low) & (lb < low + 8)) | ((lb >= 53 + low) & (lb < 61 + low))
            first = inside & (sub >= 6)
            for t in range(4, 16):
                st[dst_c, slot, w, nat(t), :] = jnp.where(
                    first if t == 4 else inside, turned[SUBS * t:SUBS * t + 8, :] * side_sign, st[dst_c, slot, w, nat(t), :])

    def vertex_rows(src, slot):
        out_rows = []
        for m in PAIR:
            row = src[slot, 2 + m].T[8:16, :]
            row = pltpu.roll(row, 1, 0)
            vals = []
            for w in range(NW):
                r = (4 * lb + w) & 127
                vals.append(lanes_of(row, 8 * (r & 15) + (r >> 4)))
            out_rows.append(vals)
        return out_rows

    def vertex_cols(src, slot):
        rows = [[src[slot, w, pl.ds(50 + 8 * m, 8, stride=0), :] for w in range(NW)] for m in PAIR]
        return lambda m, v: lanes_of(rows[m][v % 4], 4 * sub + v // 4)

    def row_mask(w):
        return vertex & (sub == 2) & (lane < 10) & (4 * lane + w < OFF)

    def col_mask(v):
        return vertex & (lane == 9) & (sub < (3 if v < 6 else 2))

    def row(ref, pos, idx, plane):
        return pick(plane, [lanes_of(ref[w, at(pos - 1), :], idx) for w in range(NW)])

    def by_column(ref, pos):
        return row(ref, pos, lane >> 2, lane & 3)

    def vertex_setup(slot):
        vals = [by_column(fr[slot], 42), by_column(fr[slot], 50), by_column(kk, 50), by_column(kk, 58)]
        for i in QUADS:
            vcoef[slot, i] = jnp.where(vertex & (sub == 1) & (lane < OFF), vals[i], 0.0)

    def vertex_columns(src, slot):
        rows = [[src[slot, w, pl.ds(50 + 8 * m, 8, stride=0), :] for w in range(NW)] for m in PAIR]

        def ghosts(v):
            for m in PAIR:
                vcol[m, reg(v), :] = lanes_of(rows[m][v % 4], 4 * sub + v // 4)

        return ghosts

    def vertex_turn(src, slot):
        both = jnp.concatenate([src[slot, 2 + m, nat(t), :] for m in PAIR for t in range(5)], axis=0)
        vbuf[0, :, pl.ds(0, 80)] = both[:, :16].T[8:16, :]

    def vertex_gains(slot, s, seven, factor):
        g1 = vbuf[0]
        g2 = pltpu.roll(g1, LANES - 40, 1)
        f1, f2, k1, k2 = [vcoef[slot, i] for i in QUADS]
        inner = s * f2 * g1
        gains = (k1 * (g1 + inner + s * f1 * (seven * g1 - g2)), -k2 * inner)
        for m in PAIR:
            moved = pltpu.roll(factor * gains[m], 1, 0)
            for w in range(NW):
                vrow[m, w] = lanes_of(moved, jnp.where(lane < 32, 4 * lane + w, LANES - 1))

    def vertex_add(dst, slot):
        for m in PAIR:
            for w in range(NW):
                sl = at(48 + 8 * m)
                dst[slot, w, sl, :] = dst[slot, w, sl, :] + vrow[m, w]

    def stage(src, dst, old, slot, s, seven, last):
        end = sub == 7

        def ldx(w, p):
            return src[slot, w, at(p), :]


        def q_row(w, v):
            if v < 0:
                return ldx(w, 8 * (NV + v) - 1)
            if v >= NV:
                return jnp.where(end, pltpu.roll(ldx(w, 8 * (2 * NV - 1 - v)), HALF, 1), ldx(w, 1 + 8 * (v - NV)))
            return ldx(w, SUBS * v)

        def flux_row(w, v):
            pos = SUBS * v if v >= 0 else 8 * (NV + v) - 1
            a, b, c, d = [q_row(w, v + i) for i in (-1, 0, 1, 2)]
            return fr[slot, w, at(pos), :] * ((seven * b - a) + (seven * c - d))

        ghosts = vertex_columns(src, slot)

        def rolls(vs):
            for v in vs:
                ghosts(v)
                q0, q1, q2, q3 = [ldx(w, SUBS * v) for w in range(NW)]
                for i, val in enumerate((pltpu.roll(q3, 1, 1), pltpu.roll(q2, 1, 1), pltpu.roll(q0, LANES - 1, 1),
                                         pltpu.roll(q1, LANES - 1, 1))):
                    roll_buf[i, reg(v), :] = val

        def along_rows(w):
            win = [q_row(w, -1), q_row(w, 0), q_row(w, 1)]
            flux = flux_row(w, -1)
            mid7 = seven * win[1]
            for v in range(NV):
                sl = reg(v)
                b, c, d = win
                n = q_row(w, v + 2)
                d7 = seven * d
                f = fr[slot, w, sl, :] * ((mid7 - b) + (d7 - n))
                row_buf[w, sl, :] = (b + d) - s * (f - flux)
                flux, mid7, win = f, d7, [c, d, n]

        def along_cols(v):
            sl = reg(v)
            q = [ldx(w, SUBS * v) for w in range(NW)]
            for m in PAIR:
                q[1 - m] = jnp.where(col_mask(v), vcol[m, sl, :], q[1 - m])
            qm1, qm2, q4, q5 = [roll_buf[i, sl, :] for i in QUADS]
            q7 = [seven * x for x in q]
            left = [q7[w] - (q[w - 1] if w else qm1) for w in range(NW)]
            right = [q7[w] - (q[w + 1] if w < 3 else q4) for w in range(NW)] + [seven * q4 - q5]
            g_prev = fcm[slot, sl, :] * ((seven * qm1 - qm2) + right[0])
            for w in range(NW):
                g = fc[slot, w, sl, :] * (left[w] + right[w + 1])
                sum_col = (q[w - 1] if w else qm1) + (q[w + 1] if w < 3 else q4)
                gain = (row_buf[w, sl, :] + sum_col) - s * (g - g_prev)
                val = mm[w, sl, :] * q[w] + kk[w, sl, :] * gain
                if last:
                    val = 0.5 * (val + old[slot, w, sl, :])
                dst[slot, w, sl, :] = val
                g_prev = g

        vertex_turn(src, slot)
        rolls(range(NV))
        for w in range(NW):
            along_rows(w)
        vertex_gains(slot, s, seven, 0.5 if last else 1.0)
        for v in range(NV):
            along_cols(v)
        vertex_add(dst, slot)

    xa, wr, wc = st.at[0], st.at[1], st.at[2]

    def load():
        low_rows = half == here.ftx
        cols = [4 * lb + w - OFF for w in range(NW)]
        cols = [c + here.fty * (size - 1 - 2 * c) for c in cols]
        flip_col = signed(here.fty == 1)

        def window(t):
            for field in range(3):
                for slot in range(slots):
                    low, high = [in_ref[field, slot, at(pl.multiple_of(first, 8)), :]
                                 for first in (SUBS * t, size + 68 - SUBS * t)]
                    low, high = [low[:, :LANES], low[:, LANES:]], [rev8(high[:, :LANES]), rev8(high[:, LANES:])]
                    for w in range(NW):
                        idx = cols[w] & (LANES - 1)
                        part = [jnp.where(cols[w] < LANES, lanes_of(x[0], idx), lanes_of(x[1], idx)) for x in (low, high)]
                        val = jnp.where(low_rows, part[0], -part[1] if field == 1 else part[1])
                        st[field, slot, w, nat(t), :] = val * flip_col if field == 2 else val

        for field in range(3):
            for slot in range(slots):
                for w in range(NW):
                    for t in QUADS:
                        st[field, slot, w, nat(t), :] = jnp.zeros((SUBS, LANES), F32)
        loop(16, window, 4)

    def faces(slot):
        cst = 0.5 / 12.0 / (0.5 * C_SPEED)
        rows = vertex_rows(wc, slot)
        cols = vertex_cols(wr, slot)
        for w in range(NW):
            sl = at(40)
            wr[slot, w, sl, :] = jnp.where(row_mask(w), -rows[0][w], wr[slot, w, sl, :])
        for v in range(NV):
            sl = reg(v)
            wc[slot, 1, sl, :] = jnp.where(col_mask(v), -cols(0, v), wc[slot, 1, sl, :])

        def plane(w):
            for v in range(NV):
                sl = reg(v)
                here_w = wr[slot, w, sl, :]
                if v < NV - 1:
                    next_w = wr[slot, w, at(SUBS * v + 8), :]
                else:
                    next_w = jnp.where(sub == 7, -pltpu.roll(here_w, HALF, 1), wr[slot, w, at(1), :])
                fr[slot, w, sl, :] = cst * (here_w + next_w)

        loop(NW, plane)
        for v in range(NV):
            sl = reg(v)
            col = [wc[slot, w, sl, :] for w in range(NW)]
            col.append(pltpu.roll(col[0], LANES - 1, 1))
            for w in range(NW):
                val = cst * (col[w] + col[w + 1])
                fc[slot, w, sl, :] = val
            fcm[slot, sl, :] = pltpu.roll(val, 1, 1)

    def store(t):
        for slot in range(slots):
            rows = [st[0, slot, w, nat(t), :] for w in range(NW)]
            for top in PAIR:
                own_half = here.ftx + top * (1 - 2 * here.ftx)
                for part in PAIR:
                    col = lane + LANES * part
                    col = (col + here.fty * (size - 1 - 2 * col) + OFF) & 255
                    val = pick(col & 3, [lanes_of(v, HALF * own_half + (col >> 2)) for v in rows])
                    first = pl.multiple_of(size + 68 - SUBS * t if top else SUBS * t, 8)
                    out[slot, at(first), pl.ds(LANES * part, LANES)] = rev8(val) if top else val

    def clear(slot):
        def one(set_id):
            for qd in QUADS:
                rbuf_c[set_id, slot, qd] = jnp.zeros((SUBS, LANES), F32)
        loop(4, one)

    loop(slots, clear)
    vbuf[...] = jnp.zeros(vbuf.shape, F32)
    barrier = pltpu.get_barrier_semaphore()

    peers = 0
    for slot in range(slots):
        for qd in QUADS:
            for kind in range(3):
                device, _, _, _, stays = to(slot, qd, kind)

                @pl.when(jnp.logical_not(stays))
                def _():
                    pl.semaphore_signal(barrier, 1, device_id=device, device_id_type=MESH_ID)

                peers = peers + jnp.where(stays, 0, 1)

    for w in range(NW):
        for v in range(NV):
            sl = reg(v)
            corner = vertex & (lane < 10) & (4 * lane + w < OFF) & (16 * sub + v < OFF)
            val = jnp.where(corner, 0.0, k_in[w, sl, :])
            kk[w, sl, :] = val
            mm[w, sl, :] = jnp.where(val == 0.0, 0.0, 1.0 - 4.0 * val)
    load()
    pl.semaphore_wait(barrier, peers)

    def first_send(field):
        def one(slot):
            pack(field, slot)
            send(field, jnp.where(field == 0, 0, field + 1), slot)
        loop(slots, one)

    loop(3, first_send)

    def wind_halos(slot):
        def one(field):
            wait_all(field, field + 1, slot, False)
            wait_all(field, field + 1, slot, True)
            unpack(field + 1, field, slot)
        loop(3, one, 1)
        faces(slot)
        vertex_setup(slot)

    loop(slots, wind_halos)

    def slot_of(i):
        if tiles * tiles * 2 != len(ORDER_OF) or slots != 3:
            return i
        at = (here.pd * tiles + here.tx) * tiles + here.ty
        code = jnp.int32(0)
        for name, order in ORDERS.items():
            value = sum(int(slot) << (2 * i) for i, slot in enumerate(order))
            for pos, other_name in enumerate(ORDER_OF):
                if other_name == name:
                    code = jnp.where(at == pos, value, code)
        return (code >> (2 * i)) & 3

    def one_round(rnd):
        def one_slot(slot):
            set_id = rnd & 1
            wait_all(0, set_id, slot, False)
            unpack(set_id, 0, slot)

            def one_step(t):
                s = ws[rnd * STEPS_PER_ROUND + t]
                seven = ws[steps]
                stage(xa, xb, xa, slot, s, seven, False)
                stage(xb, xa, xa, slot, s, seven, True)

            loop(STEPS_PER_ROUND, one_step)
            wait_all(0, 0, slot, True)

            @pl.when(rnd < rounds - 1)
            def _():
                pack(0, slot)
                send(0, 1 - set_id, slot)

        loop(slots, lambda i: one_slot(slot_of(i)))

    loop(rounds, one_round)
    loop(16, store, 4)


def metric(tiles, size):
    cells = tiles * size
    step = 0.5 * math.pi / cells
    row = jnp.arange(LANES)
    row = 16 * (row % 8) + row // 8
    halves = jnp.arange(2)
    flip_x = lax.axis_index('tx') // (tiles // 2)
    flip_y = lax.axis_index('ty') // (tiles // 2)

    def square(pos, first):
        pos = pos + first * size
        pos = jnp.where(pos < 0, -1 - pos, pos)
        pos = jnp.where(pos >= cells, 2 * cells - 1 - pos, pos)
        tan = jnp.tan((pos.astype(F32) + 0.5) * step - 0.25 * math.pi)
        return tan * tan

    own = row[:, None] - OFF
    is_high = (halves[None, :] + flip_x) % 2
    sq_a = square(jnp.where(is_high == 1, size - 1 - own, own), lax.axis_index('tx'))
    sq_a = jnp.repeat(sq_a, HALF, axis=1)[None]
    col = 4 * jnp.arange(HALF)[None, :] + jnp.arange(NW)[:, None]
    own = col - OFF
    sq_b = square(jnp.where(flip_y == 1, size - 1 - own, own), lax.axis_index('ty'))
    sq_b = jnp.tile(sq_b, (1, 2))[:, None, :]
    r_sq = 1.0 + sq_a + sq_b
    val = (0.5 * C_SPEED * CFL_STEP) * (r_sq * jnp.sqrt(r_sq)) / ((1.0 + sq_a) * (1.0 + sq_b))
    first = OFF - HALO
    col = jnp.tile(col, (1, 2))[:, None, :]
    real = (row[None, :, None] >= first) & (col >= first) & (col < 4 * HALF - first)
    return jnp.where(real, val, 0.0)


def solution(mesh):
    tiles = mesh.shape['tx']
    slots = 6 // mesh.shape['panel']
    field_spec = P(('member', 'panel'), 'tx', 'ty')
    wind_spec = P('panel', 'tx', 'ty')

    def local_run(tracer, wind_a, wind_b, wind_scale):
        size = tracer.shape[1]
        steps = wind_scale.shape[0]
        padded = jnp.stack([jnp.pad(x, ((0, 0), (OFF, 6), (0, 2 * LANES - size))) for x in (tracer, wind_a, wind_b)])
        scale = jnp.concatenate([wind_scale, jnp.full((8,), 7.0, F32)])
        vmem = pl.BlockSpec(memory_space=pltpu.VMEM)
        planes = pltpu.VMEM((slots, NW, LANES, LANES), F32)
        quad = (slots, 4)
        return pl.pallas_call(
            functools.partial(kernel, tiles, steps, size),
            out_shape=jax.ShapeDtypeStruct((slots, size + OFF + 6, 2 * LANES), F32),
            in_specs=[pl.BlockSpec(memory_space=pltpu.SMEM)] + [vmem] * 2,
            out_specs=vmem,
            scratch_shapes=[
                pltpu.VMEM((3, slots, NW, LANES, LANES), F32), planes, planes, planes,
                pltpu.VMEM((slots, LANES, LANES), F32),
                pltpu.VMEM((NW, LANES, LANES), F32), pltpu.VMEM((NW, LANES, LANES), F32),
                pltpu.VMEM((slots, 4, 8, LANES), F32),
                pltpu.VMEM((4, 8, LANES), F32), pltpu.VMEM((2, LANES, LANES), F32), pltpu.VMEM((2, NW, 8, LANES), F32),
                pltpu.VMEM((4, LANES, LANES), F32), pltpu.VMEM((NW, LANES, LANES), F32),
                pltpu.VMEM((NW, HALF, LANES), F32),
                pltpu.VMEM((NW, LANES, LANES), F32),
                pltpu.VMEM((3, *quad, 2, 96, LANES), F32),
                pltpu.VMEM((3, *quad, 2, 8, LANES), F32),
                pltpu.VMEM((4, *quad, 2, HALO, LANES), F32),
                pltpu.VMEM((4, *quad, 8, LANES), F32),
                pltpu.SemaphoreType.DMA((3, *quad, 3)),
                pltpu.SemaphoreType.DMA((4, *quad, 3)),
            ],
            compiler_params=pltpu.CompilerParams(collective_id=0, has_side_effects=True, vmem_limit_bytes=60 * 2**20),
        )(scale, padded, metric(tiles, size))[:, OFF:OFF + size, :size]

    return jax.shard_map(local_run, mesh=mesh, in_specs=(field_spec, wind_spec, wind_spec, P()),
                         out_specs=field_spec, check_vma=False)
```

```python
import functools
import math
import jax
import jax.numpy as jnp
from jax import lax
from jax.experimental import pallas as pl
from jax.experimental.pallas import tpu as pltpu
from jax.sharding import PartitionSpec as P

C_SPEED = 2.5
CFL_STEP = 0.12
EDGES = ('310,100,530,420', '010,200,511,410', '110,300,521,431', '210,000,500,401', '331,130,030,231', '320,121,221,020')
EDGE_TABLE = [[[int(digit) for digit in side] for side in panel.split(',')] for panel in EDGES]

LANES = 128
NV = 16
NW = 4
OFF = 38
HALO = 32
STEPS_PER_ROUND = 8
NIBBLE = 4
SUBS = 8
VROW = 49
HALF = 64
UNROLL = 4
PAIR = range(2)
QUADS = range(4)
ORDERS = {'a': '210', 'b': '201', 'c': '120', 'd': '102'}
ORDER_OF = 'abbbaaaacccccccc' + 'bacdbacdbacdaacd'
F32 = jnp.float32
I32 = jnp.int32
MESH_ID = pl.DeviceIdType.MESH


def lane_id():
    return lax.broadcasted_iota(I32, (SUBS, LANES), 1)


def sub_id():
    return lax.broadcasted_iota(I32, (SUBS, LANES), 0)


def lanes_of(val, idx):
    return jnp.take_along_axis(val, idx, axis=1, mode="promise_in_bounds")


def rev8(val):
    return jnp.take_along_axis(val, 7 - sub_id(), axis=0, mode="promise_in_bounds")


def pick(sel, vals):
    if isinstance(sel, int):
        return vals[sel]
    out = vals[-1]
    for i in range(len(vals) - 2, -1, -1):
        out = jnp.where(sel == i, vals[i], out)
    return out


def reg(v):
    return pl.ds(SUBS * v, SUBS)


def at(pos):
    return pl.ds(pos, SUBS)


def nat(t):
    return pl.ds(HALF * (t & 1) + (t >> 1), 8, stride=8)


class Where:
    def __init__(self, tiles, panels_per_dev):
        self.n, self.lp = tiles, panels_per_dev
        self.tx, self.ty, self.pd = lax.axis_index('tx'), lax.axis_index('ty'), lax.axis_index('panel')
        self.ftx, self.fty = self.flip(self.tx), self.flip(self.ty)
        self.edge_x = self.at_edge(self.tx)
        self.edge_y = self.at_edge(self.ty)
        self.vertex = self.edge_x * self.edge_y

    def flip(self, t):
        return lax.div(t, jnp.int32(self.n // 2))

    def at_edge(self, t):
        return jnp.where(t == 0, 1, jnp.where(t == self.n - 1, 1, 0))

    @staticmethod
    def xor(a, b):
        return a + b - 2 * a * b

    def lookup(self, slot, base, bit):
        near, far = [[np_ * SUBS + e * 2 + fl for np_, e, fl in EDGE_TABLE[slot + d * self.lp][base:base + 2]] for d in PAIR]
        low = near[0] + bit * (near[1] - near[0])
        return low + self.pd * (far[0] + bit * (far[1] - far[0]) - low)

    def cross(self, slot, base, bit, along, along_half):
        code = self.lookup(slot, base, bit)
        np_, e, fl = code >> 3, (code >> 1) & 3, code & 1
        al = along + fl * (self.n - 1 - 2 * along)
        alh = self.xor(along_half, fl)
        col, end = e >> 1, e & 1
        far = end * (self.n - 1)
        tx = far + col * (al - far)
        ty = al + col * (far - al)
        hp = end + col * (alh - end)
        kp = alh + col * (end - alh)
        pd = lax.div(np_, jnp.int32(self.lp))
        return (pd, np_ - pd * self.lp, tx, ty, self.xor(hp, self.flip(tx)), self.xor(kp, self.flip(ty)), col)

    def mix(self, flag, a, b):
        return tuple(x + flag * (y - x) for x, y in zip(a, b))

    def face(self, slot, h, k, kind):
        hp, kp = self.xor(h, self.ftx), self.xor(k, self.fty)
        if kind == 0:
            tx = self.tx + 2 * hp - 1
            inner = (self.pd, slot, tx, self.ty, self.xor(1 - hp, self.flip(tx)), k, 0)
            return inner if h else self.mix(self.edge_x, inner, self.cross(slot, 0, hp, self.ty, kp))
        ty = self.ty + 2 * kp - 1
        inner = (self.pd, slot, self.tx, ty, h, self.xor(1 - kp, self.flip(ty)), 1)
        return inner if k else self.mix(self.edge_y, inner, self.cross(slot, 2, kp, self.tx, hp))

    def corner(self, slot, h, k):
        hp, kp = self.xor(h, self.ftx), self.xor(k, self.fty)
        tx, ty = self.tx + 2 * hp - 1, self.ty + 2 * kp - 1
        dest = (self.pd, slot, tx, ty, self.xor(1 - hp, self.flip(tx)), self.xor(1 - kp, self.flip(ty)), 0)
        if not k:
            d = self.cross(slot, 2, kp, tx, 1 - hp)
            dest = self.mix(self.edge_y, dest, d[:6] + (1 - d[6],))
        if not h:
            dest = self.mix(self.edge_x, dest, self.cross(slot, 0, hp, ty, 1 - kp))
        return dest


def kernel(tiles, steps, size, ws, q_in, wa_in, wb_in, k_in, out, tile_buf, st, xb, fr, fc, fcm, kk, row_scaled, col_scaled, vcoef, vturn, vback, roll_buf, row_buf, nat_buf, turn,
           strip, strip_c, rbuf, rbuf_c, send_sem, recv_sem):
    slots = out.shape[0]
    lane, sub = lane_id(), sub_id()
    lb, half = lane & 63, lane >> 6
    here = Where(tiles, slots)
    rounds = steps // STEPS_PER_ROUND
    vertex = here.vertex == 1
    xa, wr, wc = st.at[0], st.at[1], st.at[2]

    def loop(count, fn, first=0):
        def body(i, carry):
            fn(i)
            return carry
        lax.fori_loop(first, count, body, 0)

    def plan(slot, qd, kind):
        h, k = qd >> 1, qd & 1
        dest = here.corner(slot, h, k) if kind == 2 else here.face(slot, h, k, kind)
        code = dest[0]
        for i, part in enumerate((dest[1], dest[2], dest[3], 2 * dest[4] + dest[5], dest[6])):
            code = code + (part << (NIBBLE * (i + 1)))
        if kind == 2:
            if qd:
                return code
            stays = vertex
        elif (h, k)[kind]:
            return code
        else:
            stays = (dest[0] == here.pd) & (dest[2] == here.tx) & (dest[3] == here.ty)
        return code + jnp.where(stays, 1 << (6 * NIBBLE), 0)

    plans = [[[plan(slot, qd, kind) for kind in range(3)] for qd in QUADS] for slot in range(slots)]

    def code_of(slot, qd, kind):
        return pick(slot, [plans[i][qd][kind] for i in range(slots)])

    def to(slot, qd, kind):
        code = code_of(slot, qd, kind)
        pd, slot2, tx, ty, qd2, kind2 = [(code >> (NIBBLE * i)) & ((1 << NIBBLE) - 1) for i in range(6)]
        return {'panel': pd, 'tx': tx, 'ty': ty}, slot2, qd2, kind2, (code >> (6 * NIBBLE)) == 1

    def leaves(slot, qd, kind):
        return (code_of(slot, qd, kind) >> (6 * NIBBLE)) == 0

    def send(field, set_id, slot):
        for qd in QUADS:
            for kind in range(3):
                device, slot2, qd2, kind2, stays = to(slot, qd, kind)
                if kind < 2:
                    src, dst = strip.at[field, slot, qd, kind, pl.ds(SUBS, HALO)], rbuf.at[set_id, slot2, qd2, kind2]
                    sem = recv_sem.at[set_id, slot2, qd2, kind2]
                else:
                    src, dst = strip_c.at[field, slot, qd, kind2], rbuf_c.at[set_id, slot2, qd2]
                    sem = recv_sem.at[set_id, slot2, qd2, 2]

                @pl.when(jnp.logical_not(stays))
                def _():
                    pltpu.make_async_remote_copy(
                        src_ref=src, dst_ref=dst, send_sem=send_sem.at[field, slot, qd, kind], recv_sem=sem,
                        device_id=device, device_id_type=MESH_ID).start()

                if kind < 2 and (qd >> 1, qd & 1)[kind] == 0:
                    @pl.when(stays)
                    def _():
                        for g in QUADS:
                            rbuf[set_id, slot2, qd2, kind2, reg(g), :] = (
                                strip[field, slot, qd, kind, at(8 + SUBS * g), :])

    def wait_all(field, set_id, slot, sent):
        for qd in QUADS:
            for kind in range(3):
                if kind < 2:
                    src, dst = strip.at[field, slot, qd, kind, pl.ds(SUBS, HALO)], rbuf.at[set_id, slot, qd, kind]
                else:
                    src, dst = strip_c.at[field, slot, qd, 0], rbuf_c.at[set_id, slot, qd]

                def wait():
                    copy = pltpu.make_async_remote_copy(
                        src_ref=src, dst_ref=dst, send_sem=send_sem.at[field, slot, qd, kind],
                        recv_sem=recv_sem.at[set_id, slot, qd, kind],
                        device_id={'panel': here.pd, 'tx': here.tx, 'ty': here.ty}, device_id_type=MESH_ID)
                    if sent:
                        copy.wait_send()
                    else:
                        copy.wait_recv()

                if (qd == 0) if kind == 2 else ((qd >> 1, qd & 1)[kind] == 0):
                    pl.when(leaves(slot, qd, kind))(wait)
                else:
                    wait()

    def other(field):
        return jnp.where(field == 0, 0, 3 - field)

    def signed(cond):
        return jnp.where(cond, -1.0, 1.0).astype(F32)

    def pack(field, slot):
        sign_r, sign_c = signed(field == 2), signed(field == 1)
        src_c = other(field)
        line = lax.broadcasted_iota(I32, (5 * SUBS, LANES), 1)
        plane = line & 3
        rows = [jnp.concatenate([st[field, slot, w, nat(t), :] for t in range(4, 9)], axis=0) for w in range(NW)]
        for h in PAIR:
            for k in PAIR:
                idx = HALF * h + (HALF - 1 - (line >> 2) if k else line >> 2)
                val = pick(3 - plane if k else plane, [lanes_of(v, idx) for v in rows])
                strip[field, slot, 2 * h + k, 0, pl.ds(2, 5 * SUBS), :] = val * sign_r if k else val
        for w in range(NW):
            turned = jnp.concatenate([st[src_c, slot, w, nat(t), :] for t in range(16)], axis=0).T
            for h in PAIR:
                for k, first, start in ((0, 8, 2 + w), (0, 16, 34 + w), (1, 48, 5 - w), (1, 40, 37 - w)):
                    val = turned[HALF * h + first:HALF * h + first + SUBS, :]
                    strip[field, slot, 2 * h + k, 1, pl.ds(start, SUBS, stride=4), :] = rev8(val) * sign_c if k else val
        line = lax.broadcasted_iota(I32, (HALO, LANES), 1)
        for qd in QUADS:
            for ver in PAIR:
                val = lanes_of(strip[field, slot, qd, ver, pl.ds(SUBS, HALO), :], 69 - (line & 31))
                strip_c[field, slot, qd, ver] = pick(lane >> 5, [val[SUBS * g:SUBS * g + SUBS] for g in QUADS])

    def unpack(set_id, field, slot):
        dst_c = other(field)
        row_sign = [signed(field == 1), signed(field >= 1)]
        block_sign = [signed(field >= 1), signed(field == 1)]
        col_sign = [signed(field == 1), signed(field < 0)]
        line = lax.broadcasted_iota(I32, (HALO, LANES), 1)
        near = line & (HALF - 1)
        vals = []
        for qd in QUADS:
            parts = []
            for g in reversed(QUADS):
                face = rbuf[set_id, slot, qd, 0, reg(g), :] * row_sign[qd & 1]
                block = pltpu.roll(rbuf_c[set_id, slot, qd], (6 - 32 * g) % LANES, 1) * block_sign[qd & 1]
                parts.append(rev8(jnp.where(lane < OFF, block, face)))
            vals.append(jnp.concatenate(parts, axis=0))
        for w in range(NW):
            idx = jnp.where(near < 32, 4 * near + w, 255 - 4 * near - w)
            nat_buf[w, pl.ds(OFF - HALO, HALO), :] = pick(line >> 5, [lanes_of(v, idx) for v in vals])
        for w in range(NW):
            for t in range(5):
                val = nat_buf[w, reg(t), :]
                if t == 0:
                    val = jnp.where(sub >= 6, val, 0.0)
                if t == 4:
                    val = jnp.where(sub < 6, val, st[field, slot, w, nat(t), :])
                st[field, slot, w, nat(t), :] = val
        side_sign = jnp.where(lb < 32, col_sign[0], col_sign[1])
        for w in range(NW):
            low = 1 if w >= 2 else 2
            for h in PAIR:
                turn[w, at(HALF * h + low), :] = rev8(
                    rbuf[set_id, slot, 2 * h, 1, pl.ds((1, 0, 3, 2)[w], 8, stride=4), :])
                turn[w, at(HALF * h + 53 + low), :] = (
                    rbuf[set_id, slot, 2 * h + 1, 1, pl.ds((2, 3, 0, 1)[w], 8, stride=4), :])
            turned = turn[w].T
            inside = ((lb >= low) & (lb < low + 8)) | ((lb >= 53 + low) & (lb < 61 + low))
            first = inside & (sub >= 6)
            for t in range(4, 16):
                st[dst_c, slot, w, nat(t), :] = jnp.where(
                    first if t == 4 else inside, turned[SUBS * t:SUBS * t + 8, :] * side_sign, st[dst_c, slot, w, nat(t), :])

    def col_mask(v):
        return vertex & (lane == 9) & (sub < (3 if v < 4 else 2))

    def near_vertex(w):
        return vertex & (sub == 1) & (lane < OFF // NW + 1) & (NW * lane + w < OFF)

    def vertex_setup(slot):
        for w in range(NW):
            near = near_vertex(w)
            vals = [fr[slot, w, at(VROW - SUBS), :], fr[slot, w, at(VROW), :], kk[w, at(VROW), :], kk[w, at(VROW + SUBS), :]]
            for i, val in enumerate(vals):
                vcoef[slot, w, i] = jnp.where(near, val, 0.0)

    def vertex_turn(src, slot):
        for m in PAIR:
            for w in range(NW):
                for i in range(NW):
                    vturn[m, w, pl.ds(i, SUBS, stride=NW), :] = src[slot, 2 + m, reg(NW * i + w), :]
                vturn[m, w, pl.ds(9, 1), pl.ds(0, 9)] = src[slot, w, pl.ds(VROW + 1 + SUBS * m, 1), pl.ds(0, 9)]
        for m in PAIR:
            for w in range(NW):
                vback[m, w, pl.ds(0, NV), pl.ds(0, NV)] = vturn[m, w, :NV, :NV].T

    def vertex_column(src, slot, m, v, own):
        i, w = v // NW, v % NW
        val = jnp.where(col_mask(v), vback[m, w, pl.ds(i, SUBS, stride=NW), :], own)
        if v in (4, 5):
            val = jnp.where(vertex & (lane == 9) & (sub == 2), src[slot, w, reg(6 + m), :], val)
        return val

    def vertex_add(dst, slot, s, seven, factor):
        for w in range(NW):
            g1, g2 = vback[0, w, reg(1), :], vback[1, w, reg(1), :]
            f1, f2, k1, k2 = [vcoef[slot, w, i] for i in QUADS]
            inner = s * f2 * g1
            gains = (k1 * (g1 + inner + s * f1 * (seven * g1 - g2)), -k2 * inner)
            for m in PAIR:
                sl = at(VROW + SUBS * m)
                dst[slot, w, sl, :] = dst[slot, w, sl, :] + (factor * gains[m] if factor != 1 else gains[m])

    def stage(src, dst, old, slot, s, seven, last):
        def row_wind(pos):
            return row_scaled[:, at(pos), :] if last else s * fr[slot, :, at(pos), :]

        def q_row(v):
            if v < 0:
                return src[slot, :, at(SUBS * (NV + v) - 1), :]
            if v < NV:
                return src[slot, :, reg(v), :]
            beyond = pltpu.roll(src[slot, :, reg(2 * NV - 1 - v), :], HALF, 2)
            return jnp.where(sub[None] == SUBS - 1, beyond, src[slot, :, at(1 + SUBS * (v - NV)), :])

        def along_rows():
            a, b, c, d = [q_row(i - 2) for i in QUADS]
            mid7 = seven * c
            flux = (c - b) - row_wind(SUBS * NV - SUBS - 1) * ((seven * b - a) + (mid7 - d))
            for v in range(NV):
                b, c, d = (b, c, d) if v == 0 else (c, d, n)
                n = q_row(v + 2)
                d7 = seven * d
                wind = row_wind(SUBS * v)
                if not last:
                    row_scaled[:, reg(v), :] = wind
                f = (d - c) - wind * ((mid7 - b) + (d7 - n))
                row_buf[:, reg(v), :] = f - flux
                flux, mid7 = f, d7

        def chain(*parts):
            return jnp.concatenate([x if x.ndim == 3 else x[None] for x in parts], axis=0)

        def along_cols(v):
            sl = reg(v)
            own = src[slot, :, sl, :]
            q = chain(*[vertex_column(src, slot, 1 - m, v, own[m]) for m in PAIR], own[2:])
            qm2, qm1, q4, q5 = [roll_buf[i, sl, :] for i in QUADS]
            q7 = seven * q
            up = chain(q[1:], q4)
            left, right = q7 - chain(qm1, q[:3]), q7 - up
            if last:
                wind, first_wind = col_scaled[:NW, sl, :], col_scaled[NW, sl, :]
            else:
                wind, first_wind = s * fc[slot, :, sl, :], s * fcm[slot, sl, :]
                col_scaled[:NW, sl, :] = wind
                col_scaled[NW, sl, :] = first_wind
            g = (up - q) - wind * (left + chain(right[1:], seven * q4 - q5))
            first = (q[0] - qm1) - first_wind * ((seven * qm1 - qm2) + right[0])
            val = own + kk[:, sl, :] * (row_buf[:, sl, :] + (g - chain(first, g[:3])))
            dst[slot, :, sl, :] = 0.5 * (val + old[slot, :, sl, :]) if last else val

        vertex_turn(src, slot)
        for v in range(NV):
            q = src[slot, :, reg(v), :]
            roll_buf[:2, reg(v), :] = pltpu.roll(q[2:], 1, 2)
            roll_buf[2:, reg(v), :] = pltpu.roll(q[:2], LANES - 1, 2)
        along_rows()
        for v in range(NV):
            along_cols(v)
        vertex_add(dst, slot, s, seven, 0.5 if last else 1)


    inside = pl.ds(OFF, size)
    rest = size - LANES

    def rows_in(slot):
        for field, ref in enumerate((q_in, wa_in, wb_in)):
            tile_buf[field, slot, 0, inside, :] = ref[slot, :, pl.ds(0, LANES)]
            tile_buf[field, slot, 1, inside, pl.ds(0, rest)] = ref[slot, :, pl.ds(LANES, rest)]

    def rows_out(slot):
        out[slot, :, pl.ds(0, LANES)] = tile_buf[0, slot, 0, inside, :]
        out[slot, :, pl.ds(LANES, rest)] = tile_buf[0, slot, 1, inside, pl.ds(0, rest)]

    def load():
        low_rows = half == here.ftx
        cols = [4 * lb + w - OFF for w in range(NW)]
        cols = [c + here.fty * (size - 1 - 2 * c) for c in cols]
        flip_col = signed(here.fty == 1)

        tall = [jnp.concatenate([x] * (3 * slots), axis=0) for x in (*cols, low_rows.astype(I32))]

        def window(t):
            low, high = [[tile_buf[:, :, part, at(pl.multiple_of(first, SUBS)), :] for part in PAIR]
                         for first in (SUBS * t, size + 68 - SUBS * t)]
            low = [x.reshape(3 * slots * SUBS, LANES) for x in low]
            high = [jnp.concatenate([rev8(x[f, i]) * (-1.0 if f == 1 else 1.0) for f in range(3) for i in range(slots)], axis=0)
                    for x in high]
            for w in range(NW):
                idx = tall[w] & (LANES - 1)
                part = [jnp.where(tall[w] < LANES, lanes_of(x[0], idx), lanes_of(x[1], idx)) for x in (low, high)]
                val = jnp.where(tall[NW] == 1, part[0], part[1])
                for i in range(3 * slots):
                    field, one = divmod(i, slots)
                    piece = val[SUBS * i:SUBS * i + SUBS]
                    st[field, one, w, nat(t), :] = piece * flip_col if field == 2 else piece

        def blank(slot):
            for field in range(3):
                for w in range(NW):
                    for t in QUADS:
                        st[field, slot, w, nat(t), :] = jnp.zeros((SUBS, LANES), F32)

        loop(slots, blank)
        loop(slots, rows_in)
        loop(16, window, 4)

    def faces(slot):
        cst = 0.5 / 12.0 / (0.5 * C_SPEED)
        vertex_turn(wc, slot)
        for w in range(NW):
            sl = at(VROW - SUBS)
            wr[slot, w, sl, :] = jnp.where(near_vertex(w), -vback[0, w, reg(1), :], wr[slot, w, sl, :])
        vertex_turn(wr, slot)
        for v in range(SUBS):
            for u in (v, v + SUBS):
                wc[slot, 1, reg(u), :] = -vertex_column(wr, slot, 0, u, -wc[slot, 1, reg(u), :])

        def row_faces(v):
            for w in range(NW):
                fr[slot, w, reg(v), :] = cst * (wr[slot, w, reg(v), :] + wr[slot, w, reg(v + 1), :])

        def col_faces(v):
            col = [wc[slot, w, reg(v), :] for w in range(NW)]
            col.append(pltpu.roll(col[0], LANES - 1, 1))
            for w in range(NW):
                val = cst * (col[w] + col[w + 1])
                fc[slot, w, reg(v), :] = val
            fcm[slot, reg(v), :] = pltpu.roll(val, 1, 1)

        loop(NV - 1, row_faces)
        for w in range(NW):
            inner = wr[slot, w, reg(NV - 1), :]
            beyond = jnp.where(sub == SUBS - 1, -pltpu.roll(inner, HALF, 1), wr[slot, w, at(1), :])
            fr[slot, w, reg(NV - 1), :] = cst * (inner + beyond)
        loop(NV, col_faces)

    def store(t):
        rows = [jnp.concatenate([st[0, i, w, nat(t), :] for i in range(slots)], axis=0) for w in range(NW)]
        line = lax.broadcasted_iota(I32, (slots * SUBS, LANES), 1)
        for top in PAIR:
            own_half = here.ftx + top * (1 - 2 * here.ftx)
            for part in PAIR:
                col = line + LANES * part
                col = (col + here.fty * (size - 1 - 2 * col) + OFF) & 255
                val = pick(col & 3, [lanes_of(v, HALF * own_half + (col >> 2)) for v in rows])
                first = pl.multiple_of(size + 68 - SUBS * t if top else SUBS * t, SUBS)
                for i in range(slots):
                    piece = val[SUBS * i:SUBS * i + SUBS]
                    tile_buf[0, i, part, at(first), :] = rev8(piece) if top else piece

    def clear(slot):
        def one(set_id):
            for qd in QUADS:
                rbuf_c[set_id, slot, qd] = jnp.zeros((SUBS, LANES), F32)
        loop(4, one)

    loop(slots, clear)
    vback[...] = jnp.zeros(vback.shape, F32)
    barrier = pltpu.get_barrier_semaphore()

    peers = 0
    for slot in range(slots):
        for qd in QUADS:
            for kind in range(3):
                device, _, _, _, stays = to(slot, qd, kind)

                @pl.when(jnp.logical_not(stays))
                def _():
                    pl.semaphore_signal(barrier, 1, device_id=device, device_id_type=MESH_ID)

                peers = peers + jnp.where(stays, 0, 1)

    def metric_in(v):
        for w in range(NW):
            corner = vertex & (lane < OFF // NW + 1) & (NW * lane + w < OFF) & (NV * sub + v < OFF)
            kk[w, reg(v), :] = jnp.where(corner, 0.0, k_in[w, reg(v), :])

    loop(NV, metric_in)
    load()
    pl.semaphore_wait(barrier, peers)

    def slot_of(i):
        if tiles * tiles * 2 != len(ORDER_OF) or slots != 3:
            return i
        at = (here.pd * tiles + here.tx) * tiles + here.ty
        code = jnp.int32(0)
        for name, order in ORDERS.items():
            value = sum(int(slot) << (2 * i) for i, slot in enumerate(order))
            for pos, other_name in enumerate(ORDER_OF):
                if other_name == name:
                    code = jnp.where(at == pos, value, code)
        return (code >> (2 * i)) & 3

    seven = (jnp.minimum(here.tx, 0) + 7).astype(F32)

    def one_round(turn_no):
        rnd = turn_no - 1

        def one_slot(slot):
            @pl.when(rnd >= 0)
            def _():
                def arrive(field):
                    set_id = jnp.where(field == 0, rnd & 1, field + 1)
                    wait_all(field, set_id, slot, False)
                    unpack(set_id, field, slot)

                loop(jnp.where(rnd == 0, 3, 1), arrive)

                @pl.when(rnd == 0)
                def _():
                    faces(slot)
                    vertex_setup(slot)

                def one_step(t):
                    for i in range(UNROLL):
                        s = ws[rnd * STEPS_PER_ROUND + UNROLL * t + i]
                        stage(xa, xb, xa, slot, s, seven, False)
                        stage(xb, xa, xa, slot, s, seven, True)

                loop(STEPS_PER_ROUND // UNROLL, one_step)
                loop(jnp.where(rnd == 0, 3, 1), lambda field: wait_all(field, 0, slot, True))

            @pl.when(rnd < rounds - 1)
            def _():
                def leave(field):
                    pack(field, slot)
                    send(field, jnp.where(field == 0, (rnd + 1) & 1, field + 1), slot)

                loop(jnp.where(rnd < 0, 3, 1), leave)

        loop(slots, lambda i: one_slot(slot_of(i)))

    loop(rounds + 1, one_round)
    loop(16, store, 4)
    loop(slots, rows_out)


def metric(tiles, size):
    cells = tiles * size
    step = 0.5 * math.pi / cells
    row = jnp.arange(LANES)
    row = 16 * (row % 8) + row // 8
    halves = jnp.arange(2)
    flip_x = lax.axis_index('tx') // (tiles // 2)
    flip_y = lax.axis_index('ty') // (tiles // 2)

    def square(pos, first):
        pos = pos + first * size
        pos = jnp.where(pos < 0, -1 - pos, pos)
        pos = jnp.where(pos >= cells, 2 * cells - 1 - pos, pos)
        tan = jnp.tan((pos.astype(F32) + 0.5) * step - 0.25 * math.pi)
        return tan * tan

    own = row[:, None] - OFF
    is_high = (halves[None, :] + flip_x) % 2
    sq_a = square(jnp.where(is_high == 1, size - 1 - own, own), lax.axis_index('tx'))
    sq_a = jnp.repeat(sq_a, HALF, axis=1)[None]
    col = 4 * jnp.arange(HALF)[None, :] + jnp.arange(NW)[:, None]
    own = col - OFF
    sq_b = square(jnp.where(flip_y == 1, size - 1 - own, own), lax.axis_index('ty'))
    sq_b = jnp.tile(sq_b, (1, 2))[:, None, :]
    r_sq = 1.0 + sq_a + sq_b
    val = (0.5 * C_SPEED * CFL_STEP) * (r_sq * jnp.sqrt(r_sq)) / ((1.0 + sq_a) * (1.0 + sq_b))
    first = OFF - HALO
    col = jnp.tile(col, (1, 2))[:, None, :]
    real = (row[None, :, None] >= first) & (col >= first) & (col < 4 * HALF - first)
    return jnp.where(real, val, 0.0)


def solution(mesh):
    tiles = mesh.shape['tx']
    slots = 6 // mesh.shape['panel']
    field_spec = P(('member', 'panel'), 'tx', 'ty')
    wind_spec = P('panel', 'tx', 'ty')

    def local_run(tracer, wind_a, wind_b, wind_scale):
        size = tracer.shape[1]
        steps = wind_scale.shape[0]
        vmem = pl.BlockSpec(memory_space=pltpu.VMEM)
        planes = pltpu.VMEM((slots, NW, LANES, LANES), F32)
        quad = (slots, 4)
        return pl.pallas_call(
            functools.partial(kernel, tiles, steps, size),
            out_shape=jax.ShapeDtypeStruct(tracer.shape, F32),
            in_specs=[pl.BlockSpec(memory_space=pltpu.SMEM)] + [vmem] * 4,
            out_specs=vmem,
            scratch_shapes=[
                pltpu.VMEM((3, slots, 2, size + OFF + 6, LANES), F32),
                pltpu.VMEM((3, slots, NW, LANES, LANES), F32), planes, planes, planes,
                pltpu.VMEM((slots, LANES, LANES), F32),
                pltpu.VMEM((NW, LANES, LANES), F32), pltpu.VMEM((NW, LANES, LANES), F32),
                pltpu.VMEM((NW + 1, LANES, LANES), F32),
                pltpu.VMEM((slots, NW, 4, 8, LANES), F32),
                pltpu.VMEM((2, NW, 32, LANES), F32), pltpu.VMEM((2, NW, 32, LANES), F32),
                pltpu.VMEM((4, LANES, LANES), F32), pltpu.VMEM((NW, LANES, LANES), F32),
                pltpu.VMEM((NW, HALF, LANES), F32),
                pltpu.VMEM((NW, LANES, LANES), F32),
                pltpu.VMEM((3, *quad, 2, 96, LANES), F32),
                pltpu.VMEM((3, *quad, 2, 8, LANES), F32),
                pltpu.VMEM((4, *quad, 2, HALO, LANES), F32),
                pltpu.VMEM((4, *quad, 8, LANES), F32),
                pltpu.SemaphoreType.DMA((3, *quad, 3)),
                pltpu.SemaphoreType.DMA((4, *quad, 3)),
            ],
            compiler_params=pltpu.CompilerParams(collective_id=0, has_side_effects=True, vmem_limit_bytes=60 * 2**20),
        )(wind_scale, tracer, wind_a, wind_b, metric(tiles, size))

    return jax.shard_map(local_run, mesh=mesh, in_specs=(field_spec, wind_spec, wind_spec, P()),
                         out_specs=field_spec, check_vma=False)
```

```python
import functools
import math
import jax
import jax.numpy as jnp
from jax import lax
from jax.experimental import pallas as pl
from jax.experimental.pallas import tpu as pltpu
from jax.sharding import PartitionSpec as P

C_SPEED = 2.5
CFL_STEP = 0.12
EDGES = ('310,100,530,420', '010,200,511,410', '110,300,521,431', '210,000,500,401', '331,130,030,231', '320,121,221,020')
EDGE_TABLE = [[[int(digit) for digit in side] for side in panel.split(',')] for panel in EDGES]

LANES = 128
NV = 16
NW = 4
OFF = 38
HALO = 32
STEPS_PER_ROUND = 8
PLACE = 12
STAYS = 20
SUBS = 8
VROW = 49
HALF = 64
UNROLL = 4
PAIR = range(2)
QUADS = range(4)
ORDERS = {'a': '210', 'b': '201', 'c': '120', 'd': '102'}
ORDER_OF = 'abbbaaaacccccccc' + 'bacdbacdbacdaacd'
F32 = jnp.float32
I32 = jnp.int32


def lane_id():
    return lax.broadcasted_iota(I32, (SUBS, LANES), 1)


def sub_id():
    return lax.broadcasted_iota(I32, (SUBS, LANES), 0)


def lanes_of(val, idx):
    return jnp.take_along_axis(val, idx, axis=1, mode="promise_in_bounds")


def rev8(val):
    return jnp.take_along_axis(val, 7 - sub_id(), axis=0, mode="promise_in_bounds")


def pick(sel, vals):
    if isinstance(sel, int):
        return vals[sel]
    out = vals[-1]
    for i in range(len(vals) - 2, -1, -1):
        out = jnp.where(sel == i, vals[i], out)
    return out


def reg(v):
    return pl.ds(SUBS * v, SUBS)


def at(pos):
    return pl.ds(pos, SUBS)


def nat(t):
    return pl.ds(HALF * (t & 1) + (t >> 1), 8, stride=8)


class Where:
    def __init__(self, tiles, panels_per_dev):
        self.n, self.lp = tiles, panels_per_dev
        self.tx, self.ty, self.pd = lax.axis_index('tx'), lax.axis_index('ty'), lax.axis_index('panel')
        self.member, self.panel_devs = lax.axis_index('member'), 6 // panels_per_dev
        self.ftx, self.fty = self.flip(self.tx), self.flip(self.ty)
        self.edge_x = self.at_edge(self.tx)
        self.edge_y = self.at_edge(self.ty)
        self.vertex = self.edge_x * self.edge_y

    def flip(self, t):
        return lax.div(t, jnp.int32(self.n // 2))

    def at_edge(self, t):
        return jnp.where(t == 0, 1, jnp.where(t == self.n - 1, 1, 0))

    @staticmethod
    def xor(a, b):
        return a + b - 2 * a * b

    def lookup(self, slot, base, bit):
        near, far = [[np_ * SUBS + e * 2 + fl for np_, e, fl in EDGE_TABLE[slot + d * self.lp][base:base + 2]] for d in PAIR]
        low = near[0] + bit * (near[1] - near[0])
        return low + self.pd * (far[0] + bit * (far[1] - far[0]) - low)

    def cross(self, slot, base, bit, along, along_half):
        code = self.lookup(slot, base, bit)
        np_, e, fl = code >> 3, (code >> 1) & 3, code & 1
        al = along + fl * (self.n - 1 - 2 * along)
        alh = self.xor(along_half, fl)
        col, end = e >> 1, e & 1
        far = end * (self.n - 1)
        tx = far + col * (al - far)
        ty = al + col * (far - al)
        hp = end + col * (alh - end)
        kp = alh + col * (end - alh)
        pd = lax.div(np_, jnp.int32(self.lp))
        return (pd, np_ - pd * self.lp, tx, ty, self.xor(hp, self.flip(tx)), self.xor(kp, self.flip(ty)), col)

    def mix(self, flag, a, b):
        return tuple(x + flag * (y - x) for x, y in zip(a, b))

    def face(self, slot, h, k, kind):
        hp, kp = self.xor(h, self.ftx), self.xor(k, self.fty)
        if kind == 0:
            tx = self.tx + 2 * hp - 1
            inner = (self.pd, slot, tx, self.ty, self.xor(1 - hp, self.flip(tx)), k, 0)
            return inner if h else self.mix(self.edge_x, inner, self.cross(slot, 0, hp, self.ty, kp))
        ty = self.ty + 2 * kp - 1
        inner = (self.pd, slot, self.tx, ty, h, self.xor(1 - kp, self.flip(ty)), 1)
        return inner if k else self.mix(self.edge_y, inner, self.cross(slot, 2, kp, self.tx, hp))

    def corner(self, slot, h, k):
        hp, kp = self.xor(h, self.ftx), self.xor(k, self.fty)
        tx, ty = self.tx + 2 * hp - 1, self.ty + 2 * kp - 1
        dest = (self.pd, slot, tx, ty, self.xor(1 - hp, self.flip(tx)), self.xor(1 - kp, self.flip(ty)), 0)
        if not k:
            d = self.cross(slot, 2, kp, tx, 1 - hp)
            dest = self.mix(self.edge_y, dest, d[:6] + (1 - d[6],))
        if not h:
            dest = self.mix(self.edge_x, dest, self.cross(slot, 0, hp, ty, 1 - kp))
        return dest


def kernel(tiles, steps, size, ws, q_in, wa_in, wb_in, k_in, out, tile_buf, st, xb, fr, fc, fcm, kk, row_scaled, col_scaled, vcoef, vturn, vback, roll_buf, row_buf, nat_buf, turn,
           strip, strip_c, rbuf, rbuf_c, send_sem, recv_sem):
    slots = out.shape[0]
    lane, sub = lane_id(), sub_id()
    lb, half = lane & 63, lane >> 6
    here = Where(tiles, slots)
    rounds = steps // STEPS_PER_ROUND
    vertex = here.vertex == 1
    xa, wr, wc = st.at[0], st.at[1], st.at[2]

    def loop(count, fn, first=0):
        def body(i, carry):
            fn(i)
            return carry
        lax.fori_loop(first, count, body, 0)

    def plan(slot, qd, kind):
        h, k = qd >> 1, qd & 1
        pd, slot2, tx, ty, h2, k2, kind2 = here.corner(slot, h, k) if kind == 2 else here.face(slot, h, k, kind)
        place = SUBS * slot2 + 4 * h2 + 2 * k2 + kind2
        code = ((here.member * tiles + ty) * tiles + tx) * here.panel_devs + pd + (place << PLACE)
        if not may_stay(qd, kind):
            return code
        stays = vertex if kind == 2 else (pd == here.pd) & (tx == here.tx) & (ty == here.ty)
        return code + jnp.where(stays, 1 << STAYS, 0)

    def may_stay(qd, kind):
        return qd == 0 if kind == 2 else (qd >> 1, qd & 1)[kind] == 0

    plans = [[[plan(slot, qd, kind) for kind in range(3)] for qd in QUADS] for slot in range(slots)]

    def to(slot, qd, kind):
        code = pick(slot, [plans[i][qd][kind] for i in range(slots)])
        return code & ((1 << PLACE) - 1), (code >> PLACE) & ((1 << (STAYS - PLACE)) - 1), code >= 1 << STAYS

    def send(field, set_id, slot):
        for qd in QUADS:
            for kind in range(3):
                device, place, stays = to(slot, qd, kind)
                slot2 = place >> 3
                if kind < 2:
                    src, dst = strip.at[field, slot, qd, kind, pl.ds(SUBS, HALO)], rbuf.at[set_id, place]
                else:
                    src, dst = strip_c.at[field, slot, qd, place & 1], rbuf_c.at[set_id, place >> 1]

                def start():
                    pltpu.make_async_remote_copy(
                        src_ref=src, dst_ref=dst, send_sem=send_sem.at[field, slot, kind // 2],
                        recv_sem=recv_sem.at[set_id, slot2, kind // 2],
                        device_id=device, device_id_type=pl.DeviceIdType.LOGICAL).start()

                if not may_stay(qd, kind):
                    start()
                    continue
                pl.when(jnp.logical_not(stays))(start)
                if kind < 2:
                    @pl.when(stays)
                    def _():
                        for g in QUADS:
                            rbuf[set_id, place, reg(g), :] = strip[field, slot, qd, kind, at(SUBS + SUBS * g), :]

    def wait_all(field, set_id, slot, sent):
        def wait(kind, count):
            ref = rbuf.at[set_id, pl.ds(SUBS * slot, count)] if kind == 0 else rbuf_c.at[set_id, pl.ds(4 * slot, count)]
            copy = pltpu.make_async_remote_copy(
                src_ref=ref, dst_ref=ref, send_sem=send_sem.at[field, slot, kind], recv_sem=recv_sem.at[set_id, slot, kind],
                device_id=to(slot, 3, 0)[0], device_id_type=pl.DeviceIdType.LOGICAL)
            if sent:
                copy.wait_send()
            else:
                copy.wait_recv()

        some_stay = jnp.int32(0)
        for qd, kind in ((0, 0), (1, 0), (0, 1), (2, 1)):
            some_stay = some_stay + to(slot, qd, kind)[2].astype(I32)
        for stay in range(3):
            pl.when(some_stay == stay)(functools.partial(wait, 0, SUBS - stay))
        pl.when(vertex)(lambda: wait(1, 3))
        pl.when(jnp.logical_not(vertex))(lambda: wait(1, 4))

    def other(field):
        return jnp.where(field == 0, 0, 3 - field)

    def signed(cond):
        return jnp.where(cond, -1.0, 1.0).astype(F32)

    def pack(field, slot):
        sign_r, sign_c = signed(field == 2), signed(field == 1)
        src_c = other(field)
        line = lax.broadcasted_iota(I32, (5 * SUBS, LANES), 1)
        plane = line & 3
        rows = [jnp.concatenate([st[field, slot, w, nat(t), :] for t in range(4, 9)], axis=0) for w in range(NW)]
        for h in PAIR:
            for k in PAIR:
                idx = HALF * h + (HALF - 1 - (line >> 2) if k else line >> 2)
                val = pick(3 - plane if k else plane, [lanes_of(v, idx) for v in rows])
                strip[field, slot, 2 * h + k, 0, pl.ds(2, 5 * SUBS), :] = val * sign_r if k else val
        for w in range(NW):
            turned = jnp.concatenate([st[src_c, slot, w, nat(t), :] for t in range(16)], axis=0).T
            for h in PAIR:
                for k, first, start in ((0, 8, 2 + w), (0, 16, 34 + w), (1, 48, 5 - w), (1, 40, 37 - w)):
                    val = turned[HALF * h + first:HALF * h + first + SUBS, :]
                    strip[field, slot, 2 * h + k, 1, pl.ds(start, SUBS, stride=4), :] = rev8(val) * sign_c if k else val
        line = lax.broadcasted_iota(I32, (HALO, LANES), 1)
        for qd in QUADS:
            for ver in PAIR:
                val = lanes_of(strip[field, slot, qd, ver, pl.ds(SUBS, HALO), :], 69 - (line & 31))
                strip_c[field, slot, qd, ver] = pick(lane >> 5, [val[SUBS * g:SUBS * g + SUBS] for g in QUADS])

    def unpack(set_id, field, slot):
        dst_c = other(field)
        row_sign = [signed(field == 1), signed(field >= 1)]
        block_sign = [signed(field >= 1), signed(field == 1)]
        col_sign = [signed(field == 1), signed(field < 0)]
        line = lax.broadcasted_iota(I32, (HALO, LANES), 1)
        near = line & (HALF - 1)
        vals = []
        for qd in QUADS:
            parts = []
            for g in reversed(QUADS):
                face = rbuf[set_id, SUBS * slot + 2 * qd, reg(g), :] * row_sign[qd & 1]
                block = pltpu.roll(rbuf_c[set_id, 4 * slot + qd], (6 - 32 * g) % LANES, 1) * block_sign[qd & 1]
                parts.append(rev8(jnp.where(lane < OFF, block, face)))
            vals.append(jnp.concatenate(parts, axis=0))
        for w in range(NW):
            idx = jnp.where(near < 32, 4 * near + w, 255 - 4 * near - w)
            nat_buf[w, pl.ds(OFF - HALO, HALO), :] = pick(line >> 5, [lanes_of(v, idx) for v in vals])
        for w in range(NW):
            for t in range(5):
                val = nat_buf[w, reg(t), :]
                if t == 0:
                    val = jnp.where(sub >= 6, val, 0.0)
                if t == 4:
                    val = jnp.where(sub < 6, val, st[field, slot, w, nat(t), :])
                st[field, slot, w, nat(t), :] = val
        side_sign = jnp.where(lb < 32, col_sign[0], col_sign[1])
        for w in range(NW):
            low = 1 if w >= 2 else 2
            for h in PAIR:
                turn[w, at(HALF * h + low), :] = rev8(
                    rbuf.at[set_id, SUBS * slot + 4 * h + 1][pl.ds((1, 0, 3, 2)[w], 8, stride=4), :])
                turn[w, at(HALF * h + 53 + low), :] = (
                    rbuf.at[set_id, SUBS * slot + 4 * h + 3][pl.ds((2, 3, 0, 1)[w], 8, stride=4), :])
            turned = turn[w].T
            inside = ((lb >= low) & (lb < low + 8)) | ((lb >= 53 + low) & (lb < 61 + low))
            first = inside & (sub >= 6)
            for t in range(4, 16):
                st[dst_c, slot, w, nat(t), :] = jnp.where(
                    first if t == 4 else inside, turned[SUBS * t:SUBS * t + 8, :] * side_sign, st[dst_c, slot, w, nat(t), :])

    def col_mask(v):
        return vertex & (lane == 9) & (sub < (3 if v < 4 else 2))

    def near_vertex(w):
        return vertex & (sub == 1) & (lane < OFF // NW + 1) & (NW * lane + w < OFF)

    def vertex_setup(slot):
        for w in range(NW):
            near = near_vertex(w)
            vals = [fr[slot, w, at(VROW - SUBS), :], fr[slot, w, at(VROW), :], kk[w, at(VROW), :], kk[w, at(VROW + SUBS), :]]
            for i, val in enumerate(vals):
                vcoef[slot, w, i] = jnp.where(near, val, 0.0)

    def vertex_turn(src, slot):
        for m in PAIR:
            for w in range(NW):
                for i in range(NW):
                    vturn[m, w, pl.ds(i, SUBS, stride=NW), :] = src[slot, 2 + m, reg(NW * i + w), :]
                vturn[m, w, pl.ds(9, 1), pl.ds(0, 9)] = src[slot, w, pl.ds(VROW + 1 + SUBS * m, 1), pl.ds(0, 9)]
        for m in PAIR:
            for w in range(NW):
                vback[m, w, pl.ds(0, NV), pl.ds(0, NV)] = vturn[m, w, :NV, :NV].T

    def vertex_column(src, slot, m, v, own):
        i, w = v // NW, v % NW
        val = jnp.where(col_mask(v), vback[m, w, pl.ds(i, SUBS, stride=NW), :], own)
        if v in (4, 5):
            val = jnp.where(vertex & (lane == 9) & (sub == 2), src[slot, w, reg(6 + m), :], val)
        return val

    def vertex_add(dst, slot, s, seven, factor):
        for w in range(NW):
            g1, g2 = vback[0, w, reg(1), :], vback[1, w, reg(1), :]
            f1, f2, k1, k2 = [vcoef[slot, w, i] for i in QUADS]
            inner = s * f2 * g1
            gains = (k1 * (g1 + inner + s * f1 * (seven * g1 - g2)), -k2 * inner)
            for m in PAIR:
                sl = at(VROW + SUBS * m)
                dst[slot, w, sl, :] = dst[slot, w, sl, :] + (factor * gains[m] if factor != 1 else gains[m])

    def stage(src, dst, old, slot, s, seven, last):
        def row_wind(pos):
            return row_scaled[:, at(pos), :] if last else s * fr[slot, :, at(pos), :]

        def q_row(v):
            if v < 0:
                return src[slot, :, at(SUBS * (NV + v) - 1), :]
            if v < NV:
                return src[slot, :, reg(v), :]
            beyond = pltpu.roll(src[slot, :, reg(2 * NV - 1 - v), :], HALF, 2)
            return jnp.where(sub[None] == SUBS - 1, beyond, src[slot, :, at(1 + SUBS * (v - NV)), :])

        def along_rows():
            a, b, c, d = [q_row(i - 2) for i in QUADS]
            mid7 = seven * c
            flux = (c - b) - row_wind(SUBS * NV - SUBS - 1) * ((seven * b - a) + (mid7 - d))
            for v in range(NV):
                b, c, d = (b, c, d) if v == 0 else (c, d, n)
                n = q_row(v + 2)
                d7 = seven * d
                wind = row_wind(SUBS * v)
                if not last:
                    row_scaled[:, reg(v), :] = wind
                f = (d - c) - wind * ((mid7 - b) + (d7 - n))
                row_buf[:, reg(v), :] = f - flux
                flux, mid7 = f, d7

        def chain(*parts):
            return jnp.concatenate([x if x.ndim == 3 else x[None] for x in parts], axis=0)

        def along_cols(v):
            sl = reg(v)
            own = src[slot, :, sl, :]
            q = chain(*[vertex_column(src, slot, 1 - m, v, own[m]) for m in PAIR], own[2:])
            qm2, qm1, q4, q5 = [roll_buf[i, sl, :] for i in QUADS]
            q7 = seven * q
            up = chain(q[1:], q4)
            left, right = q7 - chain(qm1, q[:3]), q7 - up
            if last:
                wind, first_wind = col_scaled[:NW, sl, :], col_scaled[NW, sl, :]
            else:
                wind, first_wind = s * fc[slot, :, sl, :], s * fcm[slot, sl, :]
                col_scaled[:NW, sl, :] = wind
                col_scaled[NW, sl, :] = first_wind
            g = (up - q) - wind * (left + chain(right[1:], seven * q4 - q5))
            first = (q[0] - qm1) - first_wind * ((seven * qm1 - qm2) + right[0])
            val = own + kk[:, sl, :] * (row_buf[:, sl, :] + (g - chain(first, g[:3])))
            dst[slot, :, sl, :] = 0.5 * (val + old[slot, :, sl, :]) if last else val

        vertex_turn(src, slot)
        for v in range(NV):
            q = src[slot, :, reg(v), :]
            roll_buf[:2, reg(v), :] = pltpu.roll(q[2:], 1, 2)
            roll_buf[2:, reg(v), :] = pltpu.roll(q[:2], LANES - 1, 2)
        along_rows()
        for v in range(NV):
            along_cols(v)
        vertex_add(dst, slot, s, seven, 0.5 if last else 1)


    inside = pl.ds(OFF, size)
    rest = size - LANES

    def rows_in(slot):
        for field, ref in enumerate((q_in, wa_in, wb_in)):
            tile_buf[field, slot, 0, inside, :] = ref[slot, :, pl.ds(0, LANES)]
            tile_buf[field, slot, 1, inside, pl.ds(0, rest)] = ref[slot, :, pl.ds(LANES, rest)]

    def rows_out(slot):
        out[slot, :, pl.ds(0, LANES)] = tile_buf[0, slot, 0, inside, :]
        out[slot, :, pl.ds(LANES, rest)] = tile_buf[0, slot, 1, inside, pl.ds(0, rest)]

    def load():
        low_rows = half == here.ftx
        cols = [4 * lb + w - OFF for w in range(NW)]
        cols = [c + here.fty * (size - 1 - 2 * c) for c in cols]
        flip_col = signed(here.fty == 1)

        tall = [jnp.concatenate([x] * (3 * slots), axis=0) for x in (*cols, low_rows.astype(I32))]

        def window(t):
            low, high = [[tile_buf[:, :, part, at(pl.multiple_of(first, SUBS)), :] for part in PAIR]
                         for first in (SUBS * t, size + 68 - SUBS * t)]
            low = [x.reshape(3 * slots * SUBS, LANES) for x in low]
            high = [jnp.concatenate([rev8(x[f, i]) * (-1.0 if f == 1 else 1.0) for f in range(3) for i in range(slots)], axis=0)
                    for x in high]
            for w in range(NW):
                idx = tall[w] & (LANES - 1)
                part = [jnp.where(tall[w] < LANES, lanes_of(x[0], idx), lanes_of(x[1], idx)) for x in (low, high)]
                val = jnp.where(tall[NW] == 1, part[0], part[1])
                for i in range(3 * slots):
                    field, one = divmod(i, slots)
                    piece = val[SUBS * i:SUBS * i + SUBS]
                    st[field, one, w, nat(t), :] = piece * flip_col if field == 2 else piece

        def blank(slot):
            for field in range(3):
                for w in range(NW):
                    for t in QUADS:
                        st[field, slot, w, nat(t), :] = jnp.zeros((SUBS, LANES), F32)

        loop(slots, blank)
        loop(slots, rows_in)
        loop(16, window, 4)

    def faces(slot):
        cst = 0.5 / 12.0 / (0.5 * C_SPEED)
        vertex_turn(wc, slot)
        for w in range(NW):
            sl = at(VROW - SUBS)
            wr[slot, w, sl, :] = jnp.where(near_vertex(w), -vback[0, w, reg(1), :], wr[slot, w, sl, :])
        vertex_turn(wr, slot)
        for v in range(SUBS):
            for u in (v, v + SUBS):
                wc[slot, 1, reg(u), :] = -vertex_column(wr, slot, 0, u, -wc[slot, 1, reg(u), :])

        def row_faces(v):
            for w in range(NW):
                fr[slot, w, reg(v), :] = cst * (wr[slot, w, reg(v), :] + wr[slot, w, reg(v + 1), :])

        def col_faces(v):
            col = [wc[slot, w, reg(v), :] for w in range(NW)]
            col.append(pltpu.roll(col[0], LANES - 1, 1))
            for w in range(NW):
                val = cst * (col[w] + col[w + 1])
                fc[slot, w, reg(v), :] = val
            fcm[slot, reg(v), :] = pltpu.roll(val, 1, 1)

        loop(NV - 1, row_faces)
        for w in range(NW):
            inner = wr[slot, w, reg(NV - 1), :]
            beyond = jnp.where(sub == SUBS - 1, -pltpu.roll(inner, HALF, 1), wr[slot, w, at(1), :])
            fr[slot, w, reg(NV - 1), :] = cst * (inner + beyond)
        loop(NV, col_faces)

    def store(t):
        rows = [jnp.concatenate([st[0, i, w, nat(t), :] for i in range(slots)], axis=0) for w in range(NW)]
        line = lax.broadcasted_iota(I32, (slots * SUBS, LANES), 1)
        for top in PAIR:
            own_half = here.ftx + top * (1 - 2 * here.ftx)
            for part in PAIR:
                col = line + LANES * part
                col = (col + here.fty * (size - 1 - 2 * col) + OFF) & 255
                val = pick(col & 3, [lanes_of(v, HALF * own_half + (col >> 2)) for v in rows])
                first = pl.multiple_of(size + 68 - SUBS * t if top else SUBS * t, SUBS)
                for i in range(slots):
                    piece = val[SUBS * i:SUBS * i + SUBS]
                    tile_buf[0, i, part, at(first), :] = rev8(piece) if top else piece

    def clear(slot):
        def one(set_id):
            for qd in QUADS:
                rbuf_c[set_id, 4 * slot + qd] = jnp.zeros((SUBS, LANES), F32)
        loop(4, one)

    loop(slots, clear)
    vback[...] = jnp.zeros(vback.shape, F32)
    barrier = pltpu.get_barrier_semaphore()

    peers = 0
    for qd, kind in ((0, 0), (2, 0), (0, 1), (1, 1), (0, 2), (1, 2), (2, 2), (3, 2)):
        crosses = 0
        if kind != 1 and qd < 2:
            crosses = here.edge_x
        if kind != 0 and not qd & 1:
            crosses = crosses | here.edge_y
        for slot in range(slots):
            device, _, stays = to(slot, qd, kind)
            greets = jnp.logical_not(stays)
            if slot:
                if isinstance(crosses, int):
                    continue
                greets = greets & (crosses == 1)

            @pl.when(greets)
            def _():
                pl.semaphore_signal(barrier, 1, device_id=device, device_id_type=pl.DeviceIdType.LOGICAL)

            peers = peers + jnp.where(greets, 1, 0)

    def metric_in(v):
        for w in range(NW):
            corner = vertex & (lane < OFF // NW + 1) & (NW * lane + w < OFF) & (NV * sub + v < OFF)
            kk[w, reg(v), :] = jnp.where(corner, 0.0, k_in[w, reg(v), :])

    loop(NV, metric_in)
    load()
    pl.semaphore_wait(barrier, peers)

    def slot_of(i):
        if tiles * tiles * 2 != len(ORDER_OF) or slots != 3:
            return i
        at = (here.pd * tiles + here.tx) * tiles + here.ty
        code = jnp.int32(0)
        for name, order in ORDERS.items():
            value = sum(int(slot) << (2 * i) for i, slot in enumerate(order))
            for pos, other_name in enumerate(ORDER_OF):
                if other_name == name:
                    code = jnp.where(at == pos, value, code)
        return (code >> (2 * i)) & 3

    seven = (jnp.minimum(here.tx, 0) + 7).astype(F32)

    def one_round(turn_no):
        rnd = turn_no - 1

        def one_slot(slot):
            @pl.when(rnd >= 0)
            def _():
                def arrive(field):
                    set_id = jnp.where(field == 0, rnd & 1, field + 1)
                    wait_all(field, set_id, slot, False)
                    unpack(set_id, field, slot)

                loop(jnp.where(rnd == 0, 3, 1), arrive)

                @pl.when(rnd == 0)
                def _():
                    faces(slot)
                    vertex_setup(slot)

                def one_step(t):
                    for i in range(UNROLL):
                        s = ws[rnd * STEPS_PER_ROUND + UNROLL * t + i]
                        stage(xa, xb, xa, slot, s, seven, False)
                        stage(xb, xa, xa, slot, s, seven, True)

                loop(STEPS_PER_ROUND // UNROLL, one_step)
                loop(jnp.where(rnd == 0, 3, 1), lambda field: wait_all(field, 0, slot, True))

            @pl.when(rnd < rounds - 1)
            def _():
                def leave(field):
                    pack(field, slot)
                    send(field, jnp.where(field == 0, (rnd + 1) & 1, field + 1), slot)

                loop(jnp.where(rnd < 0, 3, 1), leave)

        loop(slots, lambda i: one_slot(slot_of(i)))

    loop(rounds + 1, one_round)
    loop(16, store, 4)
    loop(slots, rows_out)


def metric(tiles, size):
    cells = tiles * size
    step = 0.5 * math.pi / cells
    row = jnp.arange(LANES)
    row = 16 * (row % 8) + row // 8
    halves = jnp.arange(2)
    flip_x = lax.axis_index('tx') // (tiles // 2)
    flip_y = lax.axis_index('ty') // (tiles // 2)

    def square(pos, first):
        pos = pos + first * size
        pos = jnp.where(pos < 0, -1 - pos, pos)
        pos = jnp.where(pos >= cells, 2 * cells - 1 - pos, pos)
        tan = jnp.tan((pos.astype(F32) + 0.5) * step - 0.25 * math.pi)
        return tan * tan

    own = row[:, None] - OFF
    is_high = (halves[None, :] + flip_x) % 2
    sq_a = square(jnp.where(is_high == 1, size - 1 - own, own), lax.axis_index('tx'))
    sq_a = jnp.repeat(sq_a, HALF, axis=1)[None]
    col = 4 * jnp.arange(HALF)[None, :] + jnp.arange(NW)[:, None]
    own = col - OFF
    sq_b = square(jnp.where(flip_y == 1, size - 1 - own, own), lax.axis_index('ty'))
    sq_b = jnp.tile(sq_b, (1, 2))[:, None, :]
    r_sq = 1.0 + sq_a + sq_b
    val = (0.5 * C_SPEED * CFL_STEP) * (r_sq * jnp.sqrt(r_sq)) / ((1.0 + sq_a) * (1.0 + sq_b))
    first = OFF - HALO
    col = jnp.tile(col, (1, 2))[:, None, :]
    real = (row[None, :, None] >= first) & (col >= first) & (col < 4 * HALF - first)
    return jnp.where(real, val, 0.0)


def solution(mesh):
    tiles = mesh.shape['tx']
    slots = 6 // mesh.shape['panel']
    field_spec = P(('member', 'panel'), 'tx', 'ty')
    wind_spec = P('panel', 'tx', 'ty')

    def local_run(tracer, wind_a, wind_b, wind_scale):
        size = tracer.shape[1]
        steps = wind_scale.shape[0]
        vmem = pl.BlockSpec(memory_space=pltpu.VMEM)
        planes = pltpu.VMEM((slots, NW, LANES, LANES), F32)
        quad = (slots, 4)
        return pl.pallas_call(
            functools.partial(kernel, tiles, steps, size),
            out_shape=jax.ShapeDtypeStruct(tracer.shape, F32),
            in_specs=[pl.BlockSpec(memory_space=pltpu.SMEM)] + [vmem] * 4,
            out_specs=vmem,
            scratch_shapes=[
                pltpu.VMEM((3, slots, 2, size + OFF + 6, LANES), F32),
                pltpu.VMEM((3, slots, NW, LANES, LANES), F32), planes, planes, planes,
                pltpu.VMEM((slots, LANES, LANES), F32),
                pltpu.VMEM((NW, LANES, LANES), F32), pltpu.VMEM((NW, LANES, LANES), F32),
                pltpu.VMEM((NW + 1, LANES, LANES), F32),
                pltpu.VMEM((slots, NW, 4, 8, LANES), F32),
                pltpu.VMEM((2, NW, 32, LANES), F32), pltpu.VMEM((2, NW, 32, LANES), F32),
                pltpu.VMEM((4, LANES, LANES), F32), pltpu.VMEM((NW, LANES, LANES), F32),
                pltpu.VMEM((NW, HALF, LANES), F32),
                pltpu.VMEM((NW, LANES, LANES), F32),
                pltpu.VMEM((3, *quad, 2, 96, LANES), F32),
                pltpu.VMEM((3, *quad, 2, 8, LANES), F32),
                pltpu.VMEM((4, SUBS * slots, HALO, LANES), F32),
                pltpu.VMEM((4, 4 * slots, 8, LANES), F32),
                pltpu.SemaphoreType.DMA((3, slots, 2)),
                pltpu.SemaphoreType.DMA((4, slots, 2)),
            ],
            compiler_params=pltpu.CompilerParams(collective_id=0, has_side_effects=True, vmem_limit_bytes=60 * 2**20),
        )(wind_scale, tracer, wind_a, wind_b, metric(tiles, size))

    return jax.shard_map(local_run, mesh=mesh, in_specs=(field_spec, wind_spec, wind_spec, P()),
                         out_specs=field_spec, check_vma=False)
```
